8 devices in a mesh: dp: 2 (over z, y), tp: 4 (over x, core).
Axes of the slice: x: 2, y: 2, z: 1, core: 2. Of those that a mesh axis runs over, the one named last changes fastest.
Arguments:
- token_ids: int32 [128], P('dp'), parts along dimension 0
- embed_table: bfloat16 [32768, 4096], P('tp')
- norm_gain: bfloat16 [4096], replicated
- w_in: bfloat16 [4096, 14336], P(None, 'tp')
- w_out: bfloat16 [14336, 4096], P('tp')
Outputs:
- output: bfloat16 [128, 4096], P(('dp', 'tp')), parts along dimension 0
There are 2 independent parts. The reference program is written for one: setup_inputs(seed, part) draws one part's arguments, and reference() takes and returns one part's arrays. A program takes and returns all parts, laid end to end along the dimension named above; an argument that names none is the same for every part.
All inputs are finite; a program needn't handle non-finite values.
Results may differ from the reference program's by a relative error of at most 0.00789354.
Values are sent between devices in bfloat16 or wider.
A program may use at most 1 GiB of HBM per device.

```python
import math
import jax
import jax.numpy as jnp
from jax import lax

TOKENS = 64
VOCAB_SIZE = 32768
MODEL_DIM = 4096
MLP_WIDTH = 14336
RMS_EPS = 1e-6
ROW_BLOCK = math.gcd(TOKENS, 256)


def draw_token_ids(key):
    key_mix, key_low, key_all, key_first, key_last = jax.random.split(key, 5)
    choose_low = jax.random.randint(key_mix, (TOKENS,), 0, 4) == 0
    low_ids = jax.random.randint(key_low, (TOKENS,), 0, VOCAB_SIZE // 8)
    any_ids = jax.random.randint(key_all, (TOKENS,), 0, VOCAB_SIZE)
    token_ids = jnp.where(choose_low, low_ids, any_ids)
    first_pos = jax.random.randint(key_first, (), 0, TOKENS // 2)
    last_pos = jax.random.randint(key_last, (), TOKENS // 2, TOKENS)
    token_ids = token_ids.at[first_pos].set(0).at[last_pos].set(VOCAB_SIZE - 1)
    return token_ids.astype(jnp.int32)


def setup_inputs(seed: int = 0, part: int = 0) -> dict:
    base_key = jax.random.key(seed)
    key_ids = jax.random.fold_in(jax.random.fold_in(base_key, 1), part)
    key_table, key_gain, key_in, key_out = jax.random.split(jax.random.fold_in(base_key, 2), 4)
    embed_table = jax.random.normal(key_table, (VOCAB_SIZE, MODEL_DIM), jnp.float32)
    norm_gain = jax.random.uniform(key_gain, (MODEL_DIM,), jnp.float32, 0.5, 1.5)
    w_in = jax.random.normal(key_in, (MODEL_DIM, MLP_WIDTH), jnp.float32) * MODEL_DIM ** -0.5
    w_out = jax.random.normal(key_out, (MLP_WIDTH, MODEL_DIM), jnp.float32) * MLP_WIDTH ** -0.5
    return {
        "token_ids": draw_token_ids(key_ids),
        "embed_table": embed_table.astype(jnp.bfloat16),
        "norm_gain": norm_gain.astype(jnp.bfloat16),
        "w_in": w_in.astype(jnp.bfloat16),
        "w_out": w_out.astype(jnp.bfloat16),
    }


def block_forward(embed_rows, norm_gain, w_in, w_out):
    rows_f32 = embed_rows.astype(jnp.float32)
    inv_rms = lax.rsqrt(jnp.mean(rows_f32 * rows_f32, axis=-1, keepdims=True) + RMS_EPS)
    normed = (rows_f32 * inv_rms * norm_gain.astype(jnp.float32)).astype(jnp.bfloat16)
    pre_act = jnp.dot(normed, w_in, preferred_element_type=jnp.float32).astype(jnp.bfloat16)
    activated = jax.nn.gelu(pre_act.astype(jnp.float32), approximate=True).astype(jnp.bfloat16)
    mlp_sum = jnp.dot(activated, w_out, preferred_element_type=jnp.float32)
    return (rows_f32 + mlp_sum).astype(jnp.bfloat16)


def reference(token_ids, embed_table, norm_gain, w_in, w_out):
    embedded = jnp.take(embed_table, token_ids, axis=0)
    row_blocks = embedded.reshape(TOKENS // ROW_BLOCK, ROW_BLOCK, MODEL_DIM)
    outputs = lax.map(lambda row_blk: block_forward(row_blk, norm_gain, w_in, w_out), row_blocks)
    return outputs.reshape(TOKENS, MODEL_DIM)
```

```python
import jax
import jax.numpy as jnp
from jax import lax
from jax.experimental import pallas as pl
from jax.experimental.pallas import tpu as pltpu
from jax.sharding import PartitionSpec as P

RMS_EPS = 1e-6
MESH = pl.DeviceIdType.MESH
KC = 512
NC = 512


def gather_kernel(ids_ref, table_ref, gain_ref, n_ref, x_ref, buf, tgt, sem):
    tokens = ids_ref.shape[0]
    blocks = table_ref.shape[0]
    dim = table_ref.shape[2]
    first = lax.axis_index("tp") * (blocks * 8)
    for i in range(tokens):
        local = ids_ref[i] - first
        owned = (local >= 0) & (local < blocks * 8)

        @pl.when(owned)
        def _():
            pltpu.make_async_copy(
                table_ref.at[lax.shift_right_logical(local, 3)], buf.at[i], sem.at[i]
            ).start()

        @pl.when(jnp.logical_not(owned))
        def _():
            buf[i] = jnp.zeros(buf.shape[1:], buf.dtype)

        tgt[i, :] = jnp.full((128,), jnp.where(owned, i * 8 + (local & 7), -1), jnp.int32)
    for i in range(tokens):
        local = ids_ref[i] - first
        owned = (local >= 0) & (local < blocks * 8)

        @pl.when(owned)
        def _():
            pltpu.make_async_copy(table_ref.at[0], buf.at[i], sem.at[i]).wait()

    lane = lax.broadcasted_iota(jnp.int32, (tokens, 128), 1)
    want = tgt[...]
    pick = jnp.concatenate(
        [jnp.where(lane + 128 * b == want, 1.0, 0.0) for b in range(tokens * 8 // 128)], axis=1
    ).astype(jnp.bfloat16)
    rows = jnp.dot(
        pick, buf[...].reshape(tokens * 8, dim), preferred_element_type=jnp.float32
    )
    inv_rms = lax.rsqrt(jnp.mean(rows * rows, axis=-1, keepdims=True) + RMS_EPS)
    normed = (rows * inv_rms * gain_ref[...].astype(jnp.float32)).astype(jnp.bfloat16)
    rows = rows.astype(jnp.bfloat16)
    for g in range(dim // KC):
        n_ref[g] = normed[:, g * KC : (g + 1) * KC]
        x_ref[g] = rows[:, g * KC : (g + 1) * KC]


def block_kernel(
    n_ref, x_ref, w1_ref, w2_ref, out_ref,
    w1, w2, comb, mine, other, acc, hid, y, y_in, z, z_in,
    w1_sem, w2_sem, ps, pr, xs, xr, fs, fr, ys, yr, zs, zr,
):
    tp = lax.axis_index("tp")
    chip, core = tp // 2, tp % 2
    partner = {"tp": chip * 2 + (1 - core)}
    peer = {"tp": (1 - chip) * 2 + core}
    halves = n_ref.shape[0] // 2
    outs = w2.shape[0]
    my0, other0 = core * halves, (1 - core) * halves

    def w1_copy(g):
        return pltpu.make_async_copy(
            w1_ref.at[pl.ds(pl.multiple_of(g * KC, KC), KC), :], w1.at[g], w1_sem.at[g]
        )

    def w2_copy(m):
        return pltpu.make_async_copy(
            w2_ref.at[:, pl.ds(pl.multiple_of(m * NC, NC), NC)], w2.at[m], w2_sem.at[m]
        )

    def part_copy(j):
        return pltpu.make_async_remote_copy(
            n_ref.at[other0 + j], comb.at[j], ps.at[j], pr.at[j], partner, MESH
        )

    def peer_copy(j):
        return pltpu.make_async_remote_copy(
            comb.at[j], mine.at[j], xs.at[j], xr.at[j], peer, MESH
        )

    def full_copy(j):
        return pltpu.make_async_remote_copy(
            mine.at[j], other.at[j], fs.at[j], fr.at[j], partner, MESH
        )

    def y_copy(m):
        return pltpu.make_async_remote_copy(
            y.at[m, 1 - core], y_in.at[m], ys.at[m], yr.at[m], partner, MESH
        )

    def z_copy(m):
        return pltpu.make_async_remote_copy(
            z.at[m, 1 - chip], z_in.at[m], zs.at[m], zr.at[m], peer, MESH
        )

    barrier = pltpu.get_barrier_semaphore()
    for who in (partner, peer):
        pl.semaphore_signal(barrier, inc=1, device_id=who, device_id_type=MESH)
    for j in range(halves):
        w1_copy(my0 + j).start()
        w1_copy(other0 + j).start()
    for m in range(outs):
        w2_copy(m).start()
    pl.semaphore_wait(barrier, 2)

    for j in range(halves):
        part_copy(j).start()
    for j in range(halves):
        part_copy(j).wait_recv()
        comb[j] += n_ref[my0 + j]
        peer_copy(j).start()

    acc[...] = jnp.zeros_like(acc)

    @pl.loop(0, halves)
    def _(j):
        peer_copy(j).wait_recv()
        mine[j] += comb[j]
        full_copy(j).start()
        w1_copy(my0 + j).wait()
        acc[...] += jnp.dot(mine[j], w1[my0 + j], preferred_element_type=jnp.float32)
        full_copy(j).wait_recv()
        w1_copy(other0 + j).wait()
        acc[...] += jnp.dot(other[j], w1[other0 + j], preferred_element_type=jnp.float32)

    hid[...] = jax.nn.gelu(
        acc[...].astype(jnp.bfloat16).astype(jnp.float32), approximate=True
    ).astype(jnp.bfloat16)

    rows = out_ref.shape[0]

    def combine(m):
        y_copy(m).wait_recv()
        z[m] = y[m, core] + y_in[m]
        z_copy(m).start()

    def finish(m):
        z_copy(m).wait_recv()
        out_ref[:, pl.ds(pl.multiple_of(m * NC, NC), NC)] = (z[m, chip] + z_in[m]).astype(
            out_ref.dtype
        )

    @pl.loop(0, outs)
    def _(m):
        w2_copy(m).wait()
        total = x_ref[m].astype(jnp.float32) + jnp.dot(
            hid[...], w2[m], preferred_element_type=jnp.float32
        )
        for dest_core in range(2):
            for dest_chip in range(2):
                at = (dest_chip * 2 + dest_core) * rows
                y[m, dest_core, dest_chip] = total[at : at + rows]
        y_copy(m).start()

        @pl.when(m >= 1)
        def _():
            combine(m - 1)

    combine(outs - 1)

    @pl.loop(0, outs)
    def _(m):
        finish(m)

    for j in range(halves):
        part_copy(j).wait_send()
        peer_copy(j).wait_send()
        full_copy(j).wait_send()
    for m in range(outs):
        y_copy(m).wait_send()
        z_copy(m).wait_send()


def solution(mesh):
    def device_step(token_ids, table, gain, w_in, w_out):
        tokens = token_ids.shape[0]
        vocab, dim = table.shape
        width = w_in.shape[1]
        chunks, halves, outs = dim // KC, dim // KC // 2, dim // NC
        rows = tokens // 4
        vmem = pl.BlockSpec(memory_space=pltpu.VMEM)
        hbm = pl.BlockSpec(memory_space=pl.ANY)
        piece = jax.ShapeDtypeStruct((chunks, tokens, KC), jnp.bfloat16)
        normed, embedded = pl.pallas_call(
            gather_kernel,
            name="gather_norm",
            out_shape=(piece, piece),
            in_specs=[pl.BlockSpec(memory_space=pltpu.SMEM), hbm, vmem],
            out_specs=(vmem, vmem),
            scratch_shapes=[
                pltpu.VMEM((tokens, 8, dim), jnp.bfloat16),
                pltpu.VMEM((tokens, 128), jnp.int32),
                pltpu.SemaphoreType.DMA((tokens,)),
            ],
            compiler_params=pltpu.CompilerParams(vmem_limit_bytes=24 * 2**20),
        )(token_ids, table.reshape(vocab // 8, 8, dim), gain.reshape(1, dim))

        bf16, f32 = jnp.bfloat16, jnp.float32
        dma = pltpu.SemaphoreType.DMA
        return pl.pallas_call(
            block_kernel,
            name="mlp_block",
            out_shape=jax.ShapeDtypeStruct((rows, dim), bf16),
            in_specs=[vmem, vmem, hbm, hbm],
            out_specs=vmem,
            scratch_shapes=[
                pltpu.VMEM((chunks, KC, width), bf16),
                pltpu.VMEM((outs, width, NC), bf16),
                pltpu.VMEM((halves, tokens, KC), bf16),
                pltpu.VMEM((halves, tokens, KC), bf16),
                pltpu.VMEM((halves, tokens, KC), bf16),
                pltpu.VMEM((tokens, width), f32),
                pltpu.VMEM((tokens, width), bf16),
                pltpu.VMEM((outs, 2, 2, rows, NC), f32),
                pltpu.VMEM((outs, 2, rows, NC), f32),
                pltpu.VMEM((outs, 2, rows, NC), f32),
                pltpu.VMEM((outs, rows, NC), f32),
                dma((chunks,)), dma((outs,)),
                dma((halves,)), dma((halves,)),
                dma((halves,)), dma((halves,)),
                dma((halves,)), dma((halves,)),
                dma((outs,)), dma((outs,)),
                dma((outs,)), dma((outs,)),
            ],
            compiler_params=pltpu.CompilerParams(
                collective_id=0, has_side_effects=True, vmem_limit_bytes=67_043_328
            ),
        )(normed, embedded, w_in, w_out)

    return jax.shard_map(
        device_step,
        mesh=mesh,
        in_specs=(P("dp"), P("tp", None), P(), P(None, "tp"), P("tp", None)),
        out_specs=P(("dp", "tp"), None),
        check_vma=False,
    )
```

```python
import jax
import jax.numpy as jnp
from jax import lax
from jax.experimental import pallas as pl
from jax.experimental.pallas import tpu as pltpu
from jax.sharding import PartitionSpec as P

RMS_EPS = 1e-6
MESH = pl.DeviceIdType.MESH
SUB = 8


def spans(widths):
    return [(sum(widths[:i]), w) for i, w in enumerate(widths)]


ROW_CHUNKS = spans([256, 512, 512, 512, 256])
OUT_CHUNKS = spans([256] + [512] * 7 + [256])
W1_ROWS = 3072
W2_SLOTS = 7
IN_FLIGHT = 22_100_000


def gather_kernel(ids_hbm, table_ref, gain_hbm, n_ref, x_ref, ids, gain, buf, tgt, id_sem, g_sem, sem):
    tokens, dim = x_ref.shape
    blocks = table_ref.shape[0]
    first = lax.axis_index("tp") * (blocks * SUB)
    id_copy = pltpu.make_async_copy(ids_hbm, ids, id_sem)
    id_copy.start()
    gain_copy = pltpu.make_async_copy(gain_hbm, gain, g_sem)
    gain_copy.start()
    id_copy.wait()

    def local(i):
        at = ids[i] - first
        return at, (at >= 0) & (at < blocks * SUB)

    for i in range(tokens):
        at, owned = local(i)

        @pl.when(owned)
        def _():
            pltpu.make_async_copy(
                table_ref.at[lax.shift_right_logical(at, 3)], buf.at[i], sem.at[i]
            ).start()

    for i in range(tokens):
        at, owned = local(i)

        @pl.when(jnp.logical_not(owned))
        def _():
            buf[i] = jnp.zeros(buf.shape[1:], buf.dtype)

        tgt[i, :] = jnp.full((128,), jnp.where(owned, i * SUB + (at & (SUB - 1)), -1), jnp.int32)

    lane = lax.broadcasted_iota(jnp.int32, (tokens, 128), 1)
    want = tgt[...]
    pick = jnp.concatenate(
        [jnp.where(lane + 128 * b == want, 1.0, 0.0) for b in range(tokens * SUB // 128)], axis=1
    ).astype(jnp.bfloat16)
    gain_copy.wait()
    for i in range(tokens):
        at, owned = local(i)

        @pl.when(owned)
        def _():
            pltpu.make_async_copy(table_ref.at[0], buf.at[i], sem.at[i]).wait()

    rows = jnp.dot(
        pick, buf[...].reshape(tokens * SUB, dim), preferred_element_type=jnp.float32
    )
    x_ref[...] = rows.astype(jnp.bfloat16)
    inv_rms = lax.rsqrt(jnp.mean(rows * rows, axis=-1, keepdims=True) + RMS_EPS)
    scale = gain[...].astype(jnp.float32).reshape(1, dim)
    normed = (rows * inv_rms * scale).astype(jnp.bfloat16)
    for half in range(2):
        n_ref[half] = normed[:, half * (dim // 2) : (half + 1) * (dim // 2)]


def block_kernel(
    n_ref, x_ref, w1_hbm, w2_hbm, out_ref,
    w1, w2, comb, mine, other, acc, hid, y, y_in, z, z_in,
    w1_sem, w2_sem, ps, pr, xs, xr, fs, fr, ys, yr, zs, zr,
):
    tp = lax.axis_index("tp")
    chip, core = tp // 2, tp % 2
    partner = {"tp": chip * 2 + (1 - core)}
    peer = {"tp": (1 - chip) * 2 + core}
    half = n_ref.shape[2]
    width = hid.shape[1]
    rows = out_ref.shape[0]
    nrow, nout = len(ROW_CHUNKS), len(OUT_CHUNKS)

    queue = []
    at = 0
    for j, (start, size) in enumerate(ROW_CHUNKS):
        for side, which in enumerate((core, 1 - core)):
            place = at % W1_ROWS
            queue.append(("w1", size, pltpu.make_async_copy(
                w1_hbm.at[pl.ds(pl.multiple_of(which * half + start, 256), size), :],
                w1.at[pl.ds(place, size), :],
                w1_sem.at[2 * j + side],
            )))
            at += size
    for m, (start, size) in enumerate(OUT_CHUNKS):
        queue.append(("w2", 1, pltpu.make_async_copy(
            w2_hbm.at[:, pl.ds(start, size)],
            w2.at[m % W2_SLOTS, :, pl.ds(0, size)],
            w2_sem.at[m],
        )))
    sizes = [s * width * 2 for _, s in ROW_CHUNKS for _ in range(2)] + [
        s * width * 2 for _, s in OUT_CHUNKS
    ]
    state = {"next": 0, "flight": 0, "w1": W1_ROWS, "w2": W2_SLOTS}

    def pump():
        while state["next"] < len(queue):
            k = state["next"]
            kind, need, copy = queue[k]
            if state[kind] < need or state["flight"] + sizes[k] > IN_FLIGHT:
                break
            copy.start()
            state[kind] -= need
            state["flight"] += sizes[k]
            state["next"] += 1

    def arrived(k):
        queue[k][2].wait()
        state["flight"] -= sizes[k]
        pump()

    def used(k):
        state[queue[k][0]] += queue[k][1]
        pump()

    def part_copy(j):
        cols = pl.ds(*ROW_CHUNKS[j])
        return pltpu.make_async_remote_copy(
            n_ref.at[1 - core, :, cols], comb.at[:, cols], ps.at[j], pr.at[j], partner, MESH
        )

    def peer_copy(j):
        cols = pl.ds(*ROW_CHUNKS[j])
        return pltpu.make_async_remote_copy(
            comb.at[:, cols], mine.at[:, cols], xs.at[j], xr.at[j], peer, MESH
        )

    def full_copy(j):
        cols = pl.ds(*ROW_CHUNKS[j])
        return pltpu.make_async_remote_copy(
            mine.at[:, cols], other.at[:, cols], fs.at[j], fr.at[j], partner, MESH
        )

    def y_copy(m):
        cols = pl.ds(*OUT_CHUNKS[m])
        return pltpu.make_async_remote_copy(
            y.at[1 - core, :, :, cols], y_in.at[:, :, cols], ys.at[m], yr.at[m], partner, MESH
        )

    def z_copy(m):
        cols = pl.ds(*OUT_CHUNKS[m])
        return pltpu.make_async_remote_copy(
            z.at[1 - chip, :, cols], z_in.at[:, cols], zs.at[m], zr.at[m], peer, MESH
        )

    barrier = pltpu.get_barrier_semaphore()
    for who in (partner, peer):
        pl.semaphore_signal(barrier, inc=1, device_id=who, device_id_type=MESH)
    pump()
    pl.semaphore_wait(barrier, 2)

    for j in range(nrow):
        part_copy(j).start()
    for j, (start, size) in enumerate(ROW_CHUNKS):
        cols = pl.ds(start, size)
        part_copy(j).wait_recv()
        comb[:, cols] += n_ref[core, :, cols]
        peer_copy(j).start()

    place = 0
    tile = 512
    for j, (start, size) in enumerate(ROW_CHUNKS):
        cols = pl.ds(start, size)
        peer_copy(j).wait_recv()
        mine[:, cols] += comb[:, cols]
        full_copy(j).start()
        for side, src in enumerate((mine, other)):
            k = 2 * j + side
            if side:
                full_copy(j).wait_recv()
            arrived(k)
            for c in range(0, width, tile):
                part = jnp.dot(
                    src[:, cols], w1[pl.ds(place, size), pl.ds(c, tile)],
                    preferred_element_type=jnp.float32,
                )
                if k > 0:
                    part += acc[:, c : c + tile]
                if k < 2 * nrow - 1:
                    acc[:, c : c + tile] = part
                else:
                    hid[:, c : c + tile] = jax.nn.gelu(
                        part.astype(jnp.bfloat16).astype(jnp.float32), approximate=True
                    ).astype(jnp.bfloat16)
            used(k)
            place = (place + size) % W1_ROWS

    def combine(m):
        cols = pl.ds(*OUT_CHUNKS[m])
        y_copy(m).wait_recv()
        z[:, :, cols] = y[core, :, :, cols] + y_in[:, :, cols]
        z_copy(m).start()

    def finish(m):
        cols = pl.ds(*OUT_CHUNKS[m])
        z_copy(m).wait_recv()
        out_ref[:, cols] = (z[chip, :, cols] + z_in[:, cols]).astype(out_ref.dtype)

    lag, late = 2, 6
    for m in range(nout + late):
        if m < nout:
            start, size = OUT_CHUNKS[m]
            arrived(2 * nrow + m)
            total = x_ref[:, start : start + size].astype(jnp.float32) + jnp.dot(
                hid[...], w2[m % W2_SLOTS, :, :size], preferred_element_type=jnp.float32
            )
            for dest_core in range(2):
                for dest_chip in range(2):
                    at = (dest_chip * 2 + dest_core) * rows
                    y[dest_core, dest_chip, :, start : start + size] = total[at : at + rows]
            y_copy(m).start()
            used(2 * nrow + m)
        if lag <= m < nout + lag:
            combine(m - lag)
        if m >= late:
            finish(m - late)

    for j in range(nrow):
        part_copy(j).wait_send()
        peer_copy(j).wait_send()
        full_copy(j).wait_send()
    for m in range(nout):
        y_copy(m).wait_send()
        z_copy(m).wait_send()


def solution(mesh):
    def device_step(token_ids, table, gain, w_in, w_out):
        tokens = token_ids.shape[0]
        vocab, dim = table.shape
        width = w_in.shape[1]
        half, rows = dim // 2, tokens // 4
        bf16, f32 = jnp.bfloat16, jnp.float32
        dma = pltpu.SemaphoreType.DMA
        vmem = pl.BlockSpec(memory_space=pltpu.VMEM)
        hbm = pl.BlockSpec(memory_space=pl.ANY)
        normed, embedded = pl.pallas_call(
            gather_kernel,
            name="gather_norm",
            out_shape=(
                jax.ShapeDtypeStruct((2, tokens, half), bf16),
                jax.ShapeDtypeStruct((tokens, dim), bf16),
            ),
            in_specs=[hbm, hbm, hbm],
            out_specs=(vmem, vmem),
            scratch_shapes=[
                pltpu.SMEM((tokens,), jnp.int32),
                pltpu.VMEM((dim,), bf16),
                pltpu.VMEM((tokens, SUB, dim), bf16),
                pltpu.VMEM((tokens, 128), jnp.int32),
                dma, dma, dma((tokens,)),
            ],
            compiler_params=pltpu.CompilerParams(vmem_limit_bytes=24 * 2**20),
        )(
            pltpu.with_memory_space_constraint(token_ids, pltpu.HBM),
            table.reshape(vocab // SUB, SUB, dim),
            pltpu.with_memory_space_constraint(gain, pltpu.HBM),
        )

        nrow, nout = len(ROW_CHUNKS), len(OUT_CHUNKS)
        return pl.pallas_call(
            block_kernel,
            name="mlp_block",
            out_shape=jax.ShapeDtypeStruct((rows, dim), bf16),
            in_specs=[vmem, vmem, hbm, hbm],
            out_specs=vmem,
            scratch_shapes=[
                pltpu.VMEM((W1_ROWS, width), bf16),
                pltpu.VMEM((W2_SLOTS, width, 512), bf16),
                pltpu.VMEM((tokens, half), bf16),
                pltpu.VMEM((tokens, half), bf16),
                pltpu.VMEM((tokens, half), bf16),
                pltpu.VMEM((tokens, width), f32),
                pltpu.VMEM((tokens, width), bf16),
                pltpu.VMEM((2, 2, rows, dim), f32),
                pltpu.VMEM((2, rows, dim), f32),
                pltpu.VMEM((2, rows, dim), f32),
                pltpu.VMEM((rows, dim), f32),
                dma((2 * nrow,)), dma((nout,)),
                dma((nrow,)), dma((nrow,)),
                dma((nrow,)), dma((nrow,)),
                dma((nrow,)), dma((nrow,)),
                dma((nout,)), dma((nout,)),
                dma((nout,)), dma((nout,)),
            ],
            compiler_params=pltpu.CompilerParams(
                collective_id=0, has_side_effects=True, vmem_limit_bytes=51 * 2**20
            ),
        )(normed, embedded, w_in, w_out)

    return jax.shard_map(
        device_step,
        mesh=mesh,
        in_specs=(P("dp"), P("tp", None), P(), P(None, "tp"), P("tp", None)),
        out_specs=P(("dp", "tp"), None),
        check_vma=False,
    )
```

```python
import jax
import jax.numpy as jnp
from jax import lax
from jax.experimental import pallas as pl
from jax.experimental.pallas import tpu as pltpu
from jax.sharding import PartitionSpec as P

RMS_EPS = 1e-6
MESH = pl.DeviceIdType.MESH
SUB = 2


def spans(widths):
    return [(sum(widths[:i]), w) for i, w in enumerate(widths)]


ROW_CHUNKS = spans([512] * 4)
OUT_CHUNKS = spans([512] * 8)
W1_ROWS = 3072
W2_SLOTS = 6
IN_FLIGHT = 30_000_000


def padded_dot(lhs, rhs):
    rows = lhs.shape[0]
    both = jnp.concatenate([lhs, lhs], axis=0)
    return jnp.dot(both, rhs, preferred_element_type=jnp.float32)[:rows]


def gather_kernel(ids_hbm, table_ref, gain_hbm, pairs_ref, want_ref, gain_ref, ids, id_sem, g_sem, sem):
    tokens = ids.shape[0]
    shard = table_ref.shape[0]
    tp = lax.axis_index("tp")
    id_copy = pltpu.make_async_copy(ids_hbm, ids, id_sem)
    id_copy.start()
    gain_copy = pltpu.make_async_copy(gain_hbm, gain_ref, g_sem)
    gain_copy.start()
    id_copy.wait()

    def row_copy(i, at):
        return pltpu.make_async_copy(
            table_ref.at[pl.ds(at, SUB), :], pairs_ref.at[pl.ds(i * SUB, SUB), :], sem.at[i]
        )

    for i in range(tokens):
        pair = ids[i] & (shard - SUB)
        row_copy(i, pl.multiple_of(pair, SUB)).start()
    for i in range(tokens):
        at = ids[i] - tp * shard
        owned = (at >= 0) & (at < shard)
        want_ref[i, :] = jnp.full(
            (128,), jnp.where(owned, i * SUB + (at & (SUB - 1)), -1), jnp.int32
        )
    gain_copy.wait()
    for i in range(tokens):
        row_copy(i, 0).wait()


def block_kernel(
    pairs_ref, want_ref, gain_ref, w1_hbm, w2_hbm, out_ref,
    n_ref, x_ref, w1, w2, comb, mine, other, acc, hid, y, y_in, z, z_in,
    w1_sem, w2_sem, ps, pr, xs, xr, fs, fr, ys, yr, zs, zr,
):
    tp = lax.axis_index("tp")
    chip, core = tp // 2, tp % 2
    partner = {"tp": chip * 2 + (1 - core)}
    peer = {"tp": (1 - chip) * 2 + core}
    half = n_ref.shape[2]
    width = hid.shape[1]
    rows = out_ref.shape[0]
    nrow, nout = len(ROW_CHUNKS), len(OUT_CHUNKS)

    queue = []
    at = 0
    places = {}
    for j, (start, size) in enumerate(ROW_CHUNKS):
        for side, which in enumerate((core, 1 - core)):
            place = places[j, side] = at % W1_ROWS
            queue.append(("w1", size, pltpu.make_async_copy(
                w1_hbm.at[pl.ds(pl.multiple_of(which * half + start, 256), size), :],
                w1.at[pl.ds(place, size), :],
                w1_sem.at[2 * j + side],
            )))
            at += size
    for m, (start, size) in enumerate(OUT_CHUNKS):
        queue.append(("w2", 1, pltpu.make_async_copy(
            w2_hbm.at[:, pl.ds(start, size)],
            w2.at[m % W2_SLOTS, :, pl.ds(0, size)],
            w2_sem.at[m],
        )))
    sizes = [s * width * 2 for _, s in ROW_CHUNKS for _ in range(2)] + [
        s * width * 2 for _, s in OUT_CHUNKS
    ]
    state = {"next": 0, "flight": 0, "w1": W1_ROWS, "w2": W2_SLOTS}

    def pump():
        while state["next"] < len(queue):
            k = state["next"]
            kind, need, copy = queue[k]
            if state[kind] < need or state["flight"] + sizes[k] > IN_FLIGHT:
                break
            copy.start()
            state[kind] -= need
            state["flight"] += sizes[k]
            state["next"] += 1

    def arrived(k):
        queue[k][2].wait()
        state["flight"] -= sizes[k]
        pump()

    def used(k):
        state[queue[k][0]] += queue[k][1]
        pump()

    def part_copy(j):
        cols = pl.ds(*ROW_CHUNKS[j])
        return pltpu.make_async_remote_copy(
            n_ref.at[1 - core, :, cols], comb.at[:, cols], ps.at[j], pr.at[j], partner, MESH
        )

    def peer_copy(j):
        cols = pl.ds(*ROW_CHUNKS[j])
        return pltpu.make_async_remote_copy(
            comb.at[:, cols], mine.at[:, cols], xs.at[j], xr.at[j], peer, MESH
        )

    def full_copy(j):
        cols = pl.ds(*ROW_CHUNKS[j])
        return pltpu.make_async_remote_copy(
            mine.at[:, cols], other.at[:, cols], fs.at[j], fr.at[j], partner, MESH
        )

    def y_copy(m):
        cols = pl.ds(*OUT_CHUNKS[m])
        return pltpu.make_async_remote_copy(
            y.at[1 - core, :, :, cols], y_in.at[:, :, cols], ys.at[m], yr.at[m], partner, MESH
        )

    def z_copy(m):
        cols = pl.ds(*OUT_CHUNKS[m])
        return pltpu.make_async_remote_copy(
            z.at[1 - chip, :, cols], z_in.at[:, cols], zs.at[m], zr.at[m], peer, MESH
        )

    barrier = pltpu.get_barrier_semaphore()
    for who in (partner, peer):
        pl.semaphore_signal(barrier, inc=1, device_id=who, device_id_type=MESH)
    pump()

    tokens, dim = x_ref.shape
    lane = lax.broadcasted_iota(jnp.int32, (tokens, 128), 1)
    want = want_ref[...]
    pick = jnp.concatenate(
        [jnp.where(lane + 128 * b == want, 1.0, 0.0) for b in range(tokens * SUB // 128)], axis=1
    ).astype(jnp.bfloat16)
    tile = 512
    squares = jnp.zeros((tokens, 1), jnp.float32)
    for c in range(0, dim, tile):
        picked = padded_dot(pick, pairs_ref[:, c : c + tile])
        squares += jnp.sum(picked * picked, axis=-1, keepdims=True)
        x_ref[:, c : c + tile] = picked.astype(jnp.bfloat16)
    inv_rms = lax.rsqrt(squares / dim + RMS_EPS)
    for c in range(0, dim, tile):
        scale = gain_ref[c : c + tile].astype(jnp.float32).reshape(1, tile)
        n_ref[c // half, :, c % half : c % half + tile] = (
            x_ref[:, c : c + tile].astype(jnp.float32) * inv_rms * scale
        ).astype(jnp.bfloat16)
    pl.semaphore_wait(barrier, 2)

    for j in range(nrow):
        part_copy(j).start()
    for j, (start, size) in enumerate(ROW_CHUNKS):
        cols = pl.ds(start, size)
        part_copy(j).wait_recv()
        comb[:, cols] += n_ref[core, :, cols]
        peer_copy(j).start()

    def rows_dot(j, side):
        start, size = ROW_CHUNKS[j]
        cols = pl.ds(start, size)
        src = (mine, other)[side]
        if side:
            full_copy(j).wait_recv()
        arrived(2 * j + side)
        held = w1.at[pl.ds(places[j, side], size), :]
        for c in range(0, width, tile):
            part = padded_dot(src[:, cols], held[:, pl.ds(c, tile)])
            if (j, side) != (0, 0):
                part += acc[:, c : c + tile]
            if (j, side) != (nrow - 1, 1):
                acc[:, c : c + tile] = part
            else:
                hid[:, c : c + tile] = jax.nn.gelu(
                    part.astype(jnp.bfloat16).astype(jnp.float32), approximate=True
                ).astype(jnp.bfloat16)
        used(2 * j + side)

    for j, (start, size) in enumerate(ROW_CHUNKS):
        cols = pl.ds(start, size)
        peer_copy(j).wait_recv()
        mine[:, cols] += comb[:, cols]
        full_copy(j).start()
        if j:
            rows_dot(j - 1, 1)
        rows_dot(j, 0)
    rows_dot(nrow - 1, 1)

    def combine(m):
        cols = pl.ds(*OUT_CHUNKS[m])
        y_copy(m).wait_recv()
        z[:, :, cols] = y[core, :, :, cols] + y_in[:, :, cols]
        z_copy(m).start()

    def finish(m):
        cols = pl.ds(*OUT_CHUNKS[m])
        z_copy(m).wait_recv()
        out_ref[:, cols] = (z[chip, :, cols] + z_in[:, cols]).astype(out_ref.dtype)

    lag, late = 2, 6
    for m in range(nout + late):
        if m < nout:
            start, size = OUT_CHUNKS[m]
            arrived(2 * nrow + m)
            total = x_ref[:, start : start + size].astype(jnp.float32) + padded_dot(
                hid[...], w2[m % W2_SLOTS, :, :size]
            )
            for dest_core in range(2):
                for dest_chip in range(2):
                    at = (dest_chip * 2 + dest_core) * rows
                    y[dest_core, dest_chip, :, start : start + size] = total[at : at + rows]
            y_copy(m).start()
            used(2 * nrow + m)
        if lag <= m < nout + lag:
            combine(m - lag)
        if m >= late:
            finish(m - late)

    for j in range(nrow):
        part_copy(j).wait_send()
        peer_copy(j).wait_send()
        full_copy(j).wait_send()
    for m in range(nout):
        y_copy(m).wait_send()
        z_copy(m).wait_send()


def solution(mesh):
    def device_step(token_ids, table, gain, w_in, w_out):
        tokens = token_ids.shape[0]
        dim = table.shape[1]
        width = w_in.shape[1]
        half, rows = dim // 2, tokens // 4
        bf16, f32 = jnp.bfloat16, jnp.float32
        dma = pltpu.SemaphoreType.DMA
        vmem = pl.BlockSpec(memory_space=pltpu.VMEM)
        hbm = pl.BlockSpec(memory_space=pl.ANY)
        pairs, want, gains = pl.pallas_call(
            gather_kernel,
            name="gather_rows",
            out_shape=(
                jax.ShapeDtypeStruct((tokens * SUB, dim), bf16),
                jax.ShapeDtypeStruct((tokens, 128), jnp.int32),
                jax.ShapeDtypeStruct((dim,), bf16),
            ),
            in_specs=[hbm, hbm, hbm],
            out_specs=(vmem, vmem, vmem),
            scratch_shapes=[pltpu.SMEM((tokens,), jnp.int32), dma, dma, dma((tokens,))],
            compiler_params=pltpu.CompilerParams(vmem_limit_bytes=16 * 2**20),
        )(
            pltpu.with_memory_space_constraint(token_ids, pltpu.HBM),
            table,
            pltpu.with_memory_space_constraint(gain, pltpu.HBM),
        )

        nrow, nout = len(ROW_CHUNKS), len(OUT_CHUNKS)
        return pl.pallas_call(
            block_kernel,
            name="mlp_block",
            out_shape=jax.ShapeDtypeStruct((rows, dim), bf16),
            in_specs=[vmem, vmem, vmem, hbm, hbm],
            out_specs=vmem,
            scratch_shapes=[
                pltpu.VMEM((2, tokens, half), bf16),
                pltpu.VMEM((tokens, dim), bf16),
                pltpu.VMEM((W1_ROWS, width), bf16),
                pltpu.VMEM((W2_SLOTS, width, 512), bf16),
                pltpu.VMEM((tokens, half), bf16),
                pltpu.VMEM((tokens, half), bf16),
                pltpu.VMEM((tokens, half), bf16),
                pltpu.VMEM((tokens, width), f32),
                pltpu.VMEM((tokens, width), bf16),
                pltpu.VMEM((2, 2, rows, dim), f32),
                pltpu.VMEM((2, rows, dim), f32),
                pltpu.VMEM((2, rows, dim), f32),
                pltpu.VMEM((rows, dim), f32),
                dma((2 * nrow,)), dma((nout,)),
                dma((nrow,)), dma((nrow,)),
                dma((nrow,)), dma((nrow,)),
                dma((nrow,)), dma((nrow,)),
                dma((nout,)), dma((nout,)),
                dma((nout,)), dma((nout,)),
            ],
            compiler_params=pltpu.CompilerParams(
                collective_id=0, has_side_effects=True, vmem_limit_bytes=49 * 2**20
            ),
        )(pairs, want, gains, w_in, w_out)

    return jax.shard_map(
        device_step,
        mesh=mesh,
        in_specs=(P("dp"), P("tp", None), P(), P(None, "tp"), P("tp", None)),
        out_specs=P(("dp", "tp"), None),
        check_vma=False,
    )
```

```python
import jax
import jax.numpy as jnp
from jax import lax
from jax.experimental import pallas as pl
from jax.experimental.pallas import tpu as pltpu
from jax.sharding import PartitionSpec as P

RMS_EPS = 1e-6
MESH = pl.DeviceIdType.MESH
SUB = 2


def spans(widths):
    return [(sum(widths[:i]), w) for i, w in enumerate(widths)]


ROW_CHUNKS = spans([512] * 4)
OUT_CHUNKS = spans([512] * 7 + [256] * 2)
W1_ROWS = 3584
W2_SLOTS = 5
IN_FLIGHT = 34_000_000


def padded_dot(lhs, rhs):
    rows = lhs.shape[0]
    both = jnp.concatenate([lhs, lhs], axis=0)
    return jnp.dot(both, rhs, preferred_element_type=jnp.float32)[:rows]


def gather_kernel(
    ids_hbm, table_ref, gain_hbm, w1_hbm, pairs_ref, want_ref, gain_ref, early_ref,
    ids, id_sem, g_sem, sem, w_sem,
):
    tokens = ids.shape[0]
    shard = table_ref.shape[0]
    tp = lax.axis_index("tp")
    id_copy = pltpu.make_async_copy(ids_hbm, ids, id_sem)
    id_copy.start()
    gain_copy = pltpu.make_async_copy(gain_hbm, gain_ref, g_sem)
    gain_copy.start()
    first = (tp % 2) * (pairs_ref.shape[1] // 2)
    early_copy = pltpu.make_async_copy(
        w1_hbm.at[pl.ds(pl.multiple_of(first, 512), early_ref.shape[0]), :], early_ref, w_sem
    )
    early_copy.start()
    id_copy.wait()

    def row_copy(i, at):
        return pltpu.make_async_copy(
            table_ref.at[pl.ds(at, SUB), :], pairs_ref.at[pl.ds(i * SUB, SUB), :], sem.at[i]
        )

    for i in range(tokens):
        pair = ids[i] & (shard - SUB)
        row_copy(i, pl.multiple_of(pair, SUB)).start()
    for i in range(tokens):
        at = ids[i] - tp * shard
        owned = (at >= 0) & (at < shard)
        want_ref[i, :] = jnp.full(
            (128,), jnp.where(owned, i * SUB + (at & (SUB - 1)), -1), jnp.int32
        )
    gain_copy.wait()
    for i in range(tokens):
        row_copy(i, 0).wait()
    early_copy.wait()


def block_kernel(
    pairs_ref, want_ref, gain_ref, early_ref, w1_hbm, w2_hbm, out_ref,
    n_ref, x_ref, w1, w2, comb, mine, other, acc, hid, y, y_in, z, z_in,
    w1_sem, w2_sem, ps, pr, xs, xr, fs, fr, ys, yr, zs, zr,
):
    tp = lax.axis_index("tp")
    chip, core = tp // 2, tp % 2
    partner = {"tp": chip * 2 + (1 - core)}
    peer = {"tp": (1 - chip) * 2 + core}
    half = n_ref.shape[2]
    width = hid.shape[1]
    rows = out_ref.shape[0]
    nrow, nout = len(ROW_CHUNKS), len(OUT_CHUNKS)

    queue = []
    at = 0
    places = {}
    for j, (start, size) in enumerate(ROW_CHUNKS):
        for side, which in enumerate((core, 1 - core)):
            if (j, side) == (0, 0):
                continue
            place = places[j, side] = at % W1_ROWS
            queue.append(("w1", size, pltpu.make_async_copy(
                w1_hbm.at[pl.ds(pl.multiple_of(which * half + start, 256), size), :],
                w1.at[pl.ds(place, size), :],
                w1_sem.at[2 * j + side],
            )))
            at += size
    for m, (start, size) in enumerate(OUT_CHUNKS):
        queue.append(("w2", 1, pltpu.make_async_copy(
            w2_hbm.at[:, pl.ds(start, size)],
            w2.at[m % W2_SLOTS, :, pl.ds(0, size)],
            w2_sem.at[m],
        )))
    sizes = [s * width * 2 for _, s in ROW_CHUNKS for _ in range(2)][1:] + [
        s * width * 2 for _, s in OUT_CHUNKS
    ]
    state = {"next": 0, "flight": 0, "w1": W1_ROWS, "w2": W2_SLOTS}

    def pump():
        while state["next"] < len(queue):
            k = state["next"]
            kind, need, copy = queue[k]
            if state[kind] < need or state["flight"] + sizes[k] > IN_FLIGHT:
                break
            copy.start()
            state[kind] -= need
            state["flight"] += sizes[k]
            state["next"] += 1

    def arrived(k):
        queue[k][2].wait()
        state["flight"] -= sizes[k]
        pump()

    def used(k):
        state[queue[k][0]] += queue[k][1]
        pump()

    def part_copy(j):
        cols = pl.ds(*ROW_CHUNKS[j])
        return pltpu.make_async_remote_copy(
            n_ref.at[1 - core, :, cols], comb.at[:, cols], ps.at[j], pr.at[j], partner, MESH
        )

    def peer_copy(j):
        cols = pl.ds(*ROW_CHUNKS[j])
        return pltpu.make_async_remote_copy(
            comb.at[:, cols], mine.at[:, cols], xs.at[j], xr.at[j], peer, MESH
        )

    def full_copy(j):
        cols = pl.ds(*ROW_CHUNKS[j])
        return pltpu.make_async_remote_copy(
            mine.at[:, cols], other.at[:, cols], fs.at[j], fr.at[j], partner, MESH
        )

    def y_copy(m):
        cols = pl.ds(*OUT_CHUNKS[m])
        return pltpu.make_async_remote_copy(
            y.at[1 - core, :, :, cols], y_in.at[:, :, cols], ys.at[m], yr.at[m], partner, MESH
        )

    def z_copy(m):
        cols = pl.ds(*OUT_CHUNKS[m])
        return pltpu.make_async_remote_copy(
            z.at[1 - chip, :, cols], z_in.at[:, cols], zs.at[m], zr.at[m], peer, MESH
        )

    barrier = pltpu.get_barrier_semaphore()
    for who in (partner, peer):
        pl.semaphore_signal(barrier, inc=1, device_id=who, device_id_type=MESH)
    pump()

    tokens, dim = x_ref.shape
    lane = lax.broadcasted_iota(jnp.int32, (tokens, 128), 1)
    want = want_ref[...]
    pick = jnp.concatenate(
        [jnp.where(lane + 128 * b == want, 1.0, 0.0) for b in range(tokens * SUB // 128)], axis=1
    ).astype(jnp.bfloat16)
    tile = 512
    squares = jnp.zeros((tokens, 128), jnp.float32)
    for c in range(0, dim, tile):
        picked = padded_dot(pick, pairs_ref[:, c : c + tile])
        for lanes in range(0, tile, 128):
            squares += picked[:, lanes : lanes + 128] * picked[:, lanes : lanes + 128]
        x_ref[:, c : c + tile] = picked.astype(jnp.bfloat16)
    inv_rms = lax.rsqrt(jnp.sum(squares, axis=-1, keepdims=True) / dim + RMS_EPS)

    def normalize(side, start, size):
        at = pl.ds(pl.multiple_of(side * half + start, 128), size)
        scale = gain_ref[at].astype(jnp.float32).reshape(1, size)
        n_ref[side, :, start : start + size] = (
            x_ref[:, at].astype(jnp.float32) * inv_rms * scale
        ).astype(jnp.bfloat16)

    pl.semaphore_wait(barrier, 2)
    for j, (start, size) in enumerate(ROW_CHUNKS):
        normalize(1 - core, start, size)
        part_copy(j).start()
    for start, size in ROW_CHUNKS:
        normalize(core, start, size)
    for j, (start, size) in enumerate(ROW_CHUNKS):
        cols = pl.ds(start, size)
        part_copy(j).wait_recv()
        comb[:, cols] += n_ref[core, :, cols]
        peer_copy(j).start()

    def rows_dot(j, side):
        start, size = ROW_CHUNKS[j]
        cols = pl.ds(start, size)
        src = (mine, other)[side]
        if side:
            full_copy(j).wait_recv()
        if (j, side) == (0, 0):
            held = early_ref
        else:
            arrived(2 * j + side - 1)
            held = w1.at[pl.ds(places[j, side], size), :]
        for c in range(0, width, tile):
            part = padded_dot(src[:, cols], held[:, pl.ds(c, tile)])
            if (j, side) != (0, 0):
                part += acc[:, c : c + tile]
            if (j, side) != (nrow - 1, 1):
                acc[:, c : c + tile] = part
            else:
                hid[:, c : c + tile] = jax.nn.gelu(
                    part.astype(jnp.bfloat16).astype(jnp.float32), approximate=True
                ).astype(jnp.bfloat16)
        if (j, side) != (0, 0):
            used(2 * j + side - 1)

    for j, (start, size) in enumerate(ROW_CHUNKS):
        cols = pl.ds(start, size)
        peer_copy(j).wait_recv()
        mine[:, cols] += comb[:, cols]
        full_copy(j).start()
        if j:
            rows_dot(j - 1, 1)
        rows_dot(j, 0)
    rows_dot(nrow - 1, 1)

    def combine(m):
        cols = pl.ds(*OUT_CHUNKS[m])
        y_copy(m).wait_recv()
        z[:, :, cols] = y[core, :, :, cols] + y_in[:, :, cols]
        z_copy(m).start()

    def finish(m):
        cols = pl.ds(*OUT_CHUNKS[m])
        z_copy(m).wait_recv()
        out_ref[:, cols] = (z[chip, :, cols] + z_in[:, cols]).astype(out_ref.dtype)

    lag, late = 2, 6
    for m in range(nout + late):
        if m < nout:
            start, size = OUT_CHUNKS[m]
            arrived(2 * nrow - 1 + m)
            total = x_ref[:, start : start + size].astype(jnp.float32) + padded_dot(
                hid[...], w2[m % W2_SLOTS, :, :size]
            )
            for dest_core in range(2):
                for dest_chip in range(2):
                    at = (dest_chip * 2 + dest_core) * rows
                    y[dest_core, dest_chip, :, start : start + size] = total[at : at + rows]
            y_copy(m).start()
            used(2 * nrow - 1 + m)
        if lag <= m < nout + lag:
            combine(m - lag)
        if m >= late:
            finish(m - late)

    for j in range(nrow):
        part_copy(j).wait_send()
        peer_copy(j).wait_send()
        full_copy(j).wait_send()
    for m in range(nout):
        y_copy(m).wait_send()
        z_copy(m).wait_send()


def solution(mesh):
    def device_step(token_ids, table, gain, w_in, w_out):
        tokens = token_ids.shape[0]
        dim = table.shape[1]
        width = w_in.shape[1]
        half, rows = dim // 2, tokens // 4
        bf16, f32 = jnp.bfloat16, jnp.float32
        dma = pltpu.SemaphoreType.DMA
        vmem = pl.BlockSpec(memory_space=pltpu.VMEM)
        hbm = pl.BlockSpec(memory_space=pl.ANY)
        pairs, want, gains, early = pl.pallas_call(
            gather_kernel,
            name="gather_rows",
            out_shape=(
                jax.ShapeDtypeStruct((tokens * SUB, dim), bf16),
                jax.ShapeDtypeStruct((tokens, 128), jnp.int32),
                jax.ShapeDtypeStruct((dim,), bf16),
                jax.ShapeDtypeStruct((ROW_CHUNKS[0][1], width), bf16),
            ),
            in_specs=[hbm, hbm, hbm, hbm],
            out_specs=(vmem, vmem, vmem, vmem),
            scratch_shapes=[pltpu.SMEM((tokens,), jnp.int32), dma, dma, dma((tokens,)), dma],
            compiler_params=pltpu.CompilerParams(vmem_limit_bytes=16 * 2**20),
        )(
            pltpu.with_memory_space_constraint(token_ids, pltpu.HBM),
            table,
            pltpu.with_memory_space_constraint(gain, pltpu.HBM),
            pltpu.with_memory_space_constraint(w_in, pltpu.HBM),
        )

        nrow, nout = len(ROW_CHUNKS), len(OUT_CHUNKS)
        return pl.pallas_call(
            block_kernel,
            name="mlp_block",
            out_shape=jax.ShapeDtypeStruct((rows, dim), bf16),
            in_specs=[vmem, vmem, vmem, vmem, hbm, hbm],
            out_specs=vmem,
            scratch_shapes=[
                pltpu.VMEM((2, tokens, half), bf16),
                pltpu.VMEM((tokens, dim), bf16),
                pltpu.VMEM((W1_ROWS, width), bf16),
                pltpu.VMEM((W2_SLOTS, width, 512), bf16),
                pltpu.VMEM((tokens, half), bf16),
                pltpu.VMEM((tokens, half), bf16),
                pltpu.VMEM((tokens, half), bf16),
                pltpu.VMEM((tokens, width), f32),
                pltpu.VMEM((tokens, width), bf16),
                pltpu.VMEM((2, 2, rows, dim), f32),
                pltpu.VMEM((2, rows, dim), f32),
                pltpu.VMEM((2, rows, dim), f32),
                pltpu.VMEM((rows, dim), f32),
                dma((2 * nrow,)), dma((nout,)),
                dma((nrow,)), dma((nrow,)),
                dma((nrow,)), dma((nrow,)),
                dma((nrow,)), dma((nrow,)),
                dma((nout,)), dma((nout,)),
                dma((nout,)), dma((nout,)),
            ],
            compiler_params=pltpu.CompilerParams(
                collective_id=0, has_side_effects=True, vmem_limit_bytes=97 * 2**19
            ),
        )(pairs, want, gains, early, w_in, w_out)

    return jax.shard_map(
        device_step,
        mesh=mesh,
        in_specs=(P("dp"), P("tp", None), P(), P(None, "tp"), P("tp", None)),
        out_specs=P(("dp", "tp"), None),
        check_vma=False,
    )
```

```python
import jax
import jax.numpy as jnp
from jax import lax
from jax.experimental import pallas as pl
from jax.experimental.pallas import tpu as pltpu
from jax.sharding import PartitionSpec as P

RMS_EPS = 1e-6
MESH = pl.DeviceIdType.MESH
SUB = 2


def spans(widths):
    return [(sum(widths[:i]), w) for i, w in enumerate(widths)]


ROW_CHUNKS = spans([512] * 4)
OUT_CHUNKS = spans([512] * 7 + [256] * 2)
W1_ROWS = 3584
W2_SLOTS = 5
IN_FLIGHT = 34_000_000


def padded_dot(lhs, rhs):
    rows = lhs.shape[0]
    both = jnp.concatenate([lhs, lhs], axis=0)
    return jnp.dot(both, rhs, preferred_element_type=jnp.float32)[:rows]


def gather_kernel(
    ids_hbm, table_ref, gain_hbm, w1_hbm, pairs_ref, want_ref, gain_ref, early_ref,
    ids, id_sem, g_sem, sem, w_sem,
):
    tokens = ids.shape[0]
    shard = table_ref.shape[0]
    tp = lax.axis_index("tp")
    id_copy = pltpu.make_async_copy(ids_hbm, ids, id_sem)
    id_copy.start()
    gain_copy = pltpu.make_async_copy(gain_hbm, gain_ref, g_sem)
    gain_copy.start()
    first = (tp % 2) * (pairs_ref.shape[1] // 2)
    early_copy = pltpu.make_async_copy(
        w1_hbm.at[pl.ds(pl.multiple_of(first, 512), early_ref.shape[0]), :], early_ref, w_sem
    )
    early_copy.start()
    id_copy.wait()

    def row_copy(i, at):
        return pltpu.make_async_copy(
            table_ref.at[pl.ds(at, SUB), :], pairs_ref.at[pl.ds(i * SUB, SUB), :], sem.at[i]
        )

    for i in range(tokens):
        pair = ids[i] & (shard - SUB)
        row_copy(i, pl.multiple_of(pair, SUB)).start()
    for i in range(tokens):
        at = ids[i] - tp * shard
        owned = (at >= 0) & (at < shard)
        want_ref[i, :] = jnp.full(
            (128,), jnp.where(owned, i * SUB + (at & (SUB - 1)), -1), jnp.int32
        )
    gain_copy.wait()
    for i in range(tokens):
        row_copy(i, 0).wait()
    early_copy.wait()


def block_kernel(
    pairs_ref, want_ref, gain_ref, early_ref, w1_hbm, w2_hbm, out_ref,
    n_ref, x_ref, w1, w2, comb, mine, other, acc, hid, y, y_in, z, z_in,
    w1_sem, w2_sem, ps, pr, xs, xr, fs, fr, ys, yr, zs, zr,
):
    tp = lax.axis_index("tp")
    chip, core = tp // 2, tp % 2
    partner = {"tp": chip * 2 + (1 - core)}
    peer = {"tp": (1 - chip) * 2 + core}
    half = n_ref.shape[2]
    width = hid.shape[1]
    rows = out_ref.shape[0]
    nrow, nout = len(ROW_CHUNKS), len(OUT_CHUNKS)

    queue = []
    at = 0
    places = {}
    for j, (start, size) in enumerate(ROW_CHUNKS):
        for side, which in enumerate((core, 1 - core)):
            if (j, side) == (0, 0):
                continue
            place = places[j, side] = at % W1_ROWS
            queue.append(("w1", size, pltpu.make_async_copy(
                w1_hbm.at[pl.ds(pl.multiple_of(which * half + start, 256), size), :],
                w1.at[pl.ds(place, size), :],
                w1_sem.at[2 * j + side],
            )))
            at += size
    for m, (start, size) in enumerate(OUT_CHUNKS):
        queue.append(("w2", 1, pltpu.make_async_copy(
            w2_hbm.at[:, pl.ds(start, size)],
            w2.at[m % W2_SLOTS, :, pl.ds(0, size)],
            w2_sem.at[m],
        )))
    sizes = [s * width * 2 for _, s in ROW_CHUNKS for _ in range(2)][1:] + [
        s * width * 2 for _, s in OUT_CHUNKS
    ]
    state = {"next": 0, "flight": 0, "w1": W1_ROWS, "w2": W2_SLOTS}

    def pump():
        while state["next"] < len(queue):
            k = state["next"]
            kind, need, copy = queue[k]
            if state[kind] < need or state["flight"] + sizes[k] > IN_FLIGHT:
                break
            copy.start()
            state[kind] -= need
            state["flight"] += sizes[k]
            state["next"] += 1

    def arrived(k):
        queue[k][2].wait()
        state["flight"] -= sizes[k]
        pump()

    def used(k):
        state[queue[k][0]] += queue[k][1]
        pump()

    def part_copy(j):
        cols = pl.ds(*ROW_CHUNKS[j])
        return pltpu.make_async_remote_copy(
            n_ref.at[1 - core, :, cols], comb.at[:, cols], ps.at[j], pr.at[j], partner, MESH
        )

    def peer_copy(j):
        cols = pl.ds(*ROW_CHUNKS[j])
        return pltpu.make_async_remote_copy(
            comb.at[:, cols], mine.at[:, cols], xs.at[j], xr.at[j], peer, MESH
        )

    def full_copy(j):
        cols = pl.ds(*ROW_CHUNKS[j])
        return pltpu.make_async_remote_copy(
            mine.at[:, cols], other.at[:, cols], fs.at[j], fr.at[j], partner, MESH
        )

    def y_copy(m):
        cols = pl.ds(*OUT_CHUNKS[m])
        return pltpu.make_async_remote_copy(
            y.at[1 - core, :, :, cols], y_in.at[:, :, cols], ys.at[m], yr.at[m], partner, MESH
        )

    def z_copy(m):
        cols = pl.ds(*OUT_CHUNKS[m])
        return pltpu.make_async_remote_copy(
            z.at[1 - chip, :, cols], z_in.at[:, cols], zs.at[m], zr.at[m], peer, MESH
        )

    barrier = pltpu.get_barrier_semaphore()
    for who in (partner, peer):
        pl.semaphore_signal(barrier, inc=1, device_id=who, device_id_type=MESH)
    pump()

    tokens, dim = x_ref.shape
    lane = lax.broadcasted_iota(jnp.int32, (tokens, 128), 1)
    want = want_ref[...]
    pick = jnp.concatenate(
        [jnp.where(lane + 128 * b == want, 1.0, 0.0) for b in range(tokens * SUB // 128)], axis=1
    ).astype(jnp.bfloat16)
    tile = 512
    squares = jnp.zeros((tokens, 128), jnp.float32)
    for c in range(0, dim, tile):
        picked = jnp.dot(
            pick, pairs_ref[:, c : c + tile], preferred_element_type=jnp.float32
        )
        for lanes in range(0, tile, 128):
            squares += picked[:, lanes : lanes + 128] * picked[:, lanes : lanes + 128]
        x_ref[:, c : c + tile] = picked.astype(jnp.bfloat16)
    inv_rms = lax.rsqrt(jnp.sum(squares, axis=-1, keepdims=True) / dim + RMS_EPS)

    def normalize(side, start, size):
        at = pl.ds(pl.multiple_of(side * half + start, 128), size)
        scale = gain_ref[at].astype(jnp.float32).reshape(1, size)
        n_ref[side, :, start : start + size] = (
            x_ref[:, at].astype(jnp.float32) * inv_rms * scale
        ).astype(jnp.bfloat16)

    pl.semaphore_wait(barrier, 2)
    for j, (start, size) in enumerate(ROW_CHUNKS):
        normalize(1 - core, start, size)
        part_copy(j).start()
    for start, size in ROW_CHUNKS:
        normalize(core, start, size)
    for j, (start, size) in enumerate(ROW_CHUNKS):
        cols = pl.ds(start, size)
        part_copy(j).wait_recv()
        comb[:, cols] += n_ref[core, :, cols]
        peer_copy(j).start()

    def rows_dot(j, side):
        start, size = ROW_CHUNKS[j]
        cols = pl.ds(start, size)
        src = (mine, other)[side]
        if side:
            full_copy(j).wait_recv()
        if (j, side) == (0, 0):
            held = early_ref
        else:
            arrived(2 * j + side - 1)
            if (j, side) == (nrow - 1, 1):
                arrived(2 * nrow - 1)
            held = w1.at[pl.ds(places[j, side], size), :]
        for c in range(0, width, tile):
            part = padded_dot(src[:, cols], held[:, pl.ds(c, tile)])
            if (j, side) != (0, 0):
                part += acc[:, c : c + tile]
            if (j, side) != (nrow - 1, 1):
                acc[:, c : c + tile] = part
            else:
                hid[:, c : c + tile] = jax.nn.gelu(
                    part.astype(jnp.bfloat16).astype(jnp.float32), approximate=True
                ).astype(jnp.bfloat16)
        if (j, side) != (0, 0):
            used(2 * j + side - 1)

    for j, (start, size) in enumerate(ROW_CHUNKS):
        cols = pl.ds(start, size)
        peer_copy(j).wait_recv()
        mine[:, cols] += comb[:, cols]
        full_copy(j).start()
        if j:
            rows_dot(j - 1, 1)
        rows_dot(j, 0)
    rows_dot(nrow - 1, 1)

    def combine(m):
        cols = pl.ds(*OUT_CHUNKS[m])
        y_copy(m).wait_recv()
        z[:, :, cols] = y[core, :, :, cols] + y_in[:, :, cols]
        z_copy(m).start()

    def finish(m):
        cols = pl.ds(*OUT_CHUNKS[m])
        z_copy(m).wait_recv()
        out_ref[:, cols] = (z[chip, :, cols] + z_in[:, cols]).astype(out_ref.dtype)

    lag, late = 2, 6
    for m in range(nout + late):
        if m < nout:
            start, size = OUT_CHUNKS[m]
            if m > 0:
                arrived(2 * nrow - 1 + m)
            total = x_ref[:, start : start + size].astype(jnp.float32) + padded_dot(
                hid[...], w2[m % W2_SLOTS, :, :size]
            )
            for dest_core in range(2):
                for dest_chip in range(2):
                    at = (dest_chip * 2 + dest_core) * rows
                    y[dest_core, dest_chip, :, start : start + size] = total[at : at + rows]
            y_copy(m).start()
            used(2 * nrow - 1 + m)
        if lag <= m < nout + lag:
            combine(m - lag)
        if m >= late:
            finish(m - late)

    for j in range(nrow):
        part_copy(j).wait_send()
        peer_copy(j).wait_send()
        full_copy(j).wait_send()
    for m in range(nout):
        y_copy(m).wait_send()
        z_copy(m).wait_send()


def solution(mesh):
    def device_step(token_ids, table, gain, w_in, w_out):
        tokens = token_ids.shape[0]
        dim = table.shape[1]
        width = w_in.shape[1]
        half, rows = dim // 2, tokens // 4
        bf16, f32 = jnp.bfloat16, jnp.float32
        dma = pltpu.SemaphoreType.DMA
        vmem = pl.BlockSpec(memory_space=pltpu.VMEM)
        hbm = pl.BlockSpec(memory_space=pl.ANY)
        pairs, want, gains, early = pl.pallas_call(
            gather_kernel,
            name="gather_rows",
            out_shape=(
                jax.ShapeDtypeStruct((tokens * SUB, dim), bf16),
                jax.ShapeDtypeStruct((tokens, 128), jnp.int32),
                jax.ShapeDtypeStruct((dim,), bf16),
                jax.ShapeDtypeStruct((ROW_CHUNKS[0][1], width), bf16),
            ),
            in_specs=[hbm, hbm, hbm, hbm],
            out_specs=(vmem, vmem, vmem, vmem),
            scratch_shapes=[pltpu.SMEM((tokens,), jnp.int32), dma, dma, dma((tokens,)), dma],
            compiler_params=pltpu.CompilerParams(vmem_limit_bytes=16 * 2**20),
        )(
            pltpu.with_memory_space_constraint(token_ids, pltpu.HBM),
            table,
            pltpu.with_memory_space_constraint(gain, pltpu.HBM),
            pltpu.with_memory_space_constraint(w_in, pltpu.HBM),
        )

        nrow, nout = len(ROW_CHUNKS), len(OUT_CHUNKS)
        return pl.pallas_call(
            block_kernel,
            name="mlp_block",
            out_shape=jax.ShapeDtypeStruct((rows, dim), bf16),
            in_specs=[vmem, vmem, vmem, vmem, hbm, hbm],
            out_specs=vmem,
            scratch_shapes=[
                pltpu.VMEM((2, tokens, half), bf16),
                pltpu.VMEM((tokens, dim), bf16),
                pltpu.VMEM((W1_ROWS, width), bf16),
                pltpu.VMEM((W2_SLOTS, width, 512), bf16),
                pltpu.VMEM((tokens, half), bf16),
                pltpu.VMEM((tokens, half), bf16),
                pltpu.VMEM((tokens, half), bf16),
                pltpu.VMEM((tokens, width), f32),
                pltpu.VMEM((tokens, width), bf16),
                pltpu.VMEM((2, 2, rows, dim), f32),
                pltpu.VMEM((2, rows, dim), f32),
                pltpu.VMEM((2, rows, dim), f32),
                pltpu.VMEM((rows, dim), f32),
                dma((2 * nrow,)), dma((nout,)),
                dma((nrow,)), dma((nrow,)),
                dma((nrow,)), dma((nrow,)),
                dma((nrow,)), dma((nrow,)),
                dma((nout,)), dma((nout,)),
                dma((nout,)), dma((nout,)),
            ],
            compiler_params=pltpu.CompilerParams(
                collective_id=0, has_side_effects=True, vmem_limit_bytes=97 * 2**19
            ),
        )(pairs, want, gains, early, w_in, w_out)

    return jax.shard_map(
        device_step,
        mesh=mesh,
        in_specs=(P("dp"), P("tp", None), P(), P(None, "tp"), P("tp", None)),
        out_specs=P(("dp", "tp"), None),
        check_vma=False,
    )
```
